512 devices in a mesh: groups: 2 (over y), seq: 32 (over z), tp: 8 (over x, core).
Axes of the slice: x: 4, y: 2, z: 32, core: 2. Of those that a mesh axis runs over, the one named last changes fastest.
The devices are a block of a 4x8x32 slice.
Arguments:
- prompt_kv: bfloat16 [32768, 64, 128], P(('groups', 'seq', 'tp')), parts along dimension 0, may hold values from -6 to 6
- prompt_length: int32 [2], P('groups'), parts along dimension 0, may hold values from 8192 to 16384
- queries: bfloat16 [16, 4096], P('groups'), parts along dimension 0, may hold values from -6 to 6
- new_kv: bfloat16 [16, 16, 2, 128], P('groups'), parts along dimension 0, may hold values from -6 to 6
- k_cache: bfloat16 [256, 8192, 128], P(('groups', 'seq'), 'tp'), parts along dimension 0, may hold values from -6 to 6
- v_cache: bfloat16 [256, 8192, 128], P(('groups', 'seq'), 'tp'), parts along dimension 0, may hold values from -6 to 6
- lengths: int32 [16], P('groups'), parts along dimension 0, may hold values from 4097 to 8192
- slots: int32 [16], P('groups'), parts along dimension 0, may hold values from 0 to 7, each once
Outputs:
- prompt_owned: bfloat16 [32768, 64, 128], P(('groups', 'tp'), 'seq'), parts along dimension 0
- attended: bfloat16 [256, 256], P(('groups', 'seq')), parts along dimension 0
The draws below stay inside these ranges and needn't reach their ends.
There are 2 independent parts, one for each index of `groups`. The reference program is written for one: setup_inputs(seed, part) draws one part's arguments, and reference() takes and returns one part's arrays. A program takes and returns all parts, laid end to end along the dimension named above; each array names one. Nothing has to cross between parts.
Inputs may be any that keep to these rules, and one draw needn't show every extreme that they name: `slots`: each slot once.
All inputs are finite; a program needn't handle non-finite values.
Results may differ from the reference program's by a relative error of at most 0.0028.
Values may be sent and summed in bfloat16 or wider, within the bound.
A program may use at most 64 MiB of HBM per device.

```python
import jax
import jax.numpy as jnp
from jax import lax

KVH = 16
QH = 32
HD = 128
RESIDENT = 8
CACHE_LEN = 8192
PROMPT = 16384
GROUP = 2
KV_ROWS = 64
PAIRS = 128
BLOCK = 64
N_SEQ = 32
N_TP = 8


query_scale = 168.0 ** (-0.5)


cache_strength = 6.0


def common_pattern(key):
    signs = jax.random.bernoulli(jax.random.fold_in(key, 7101), 0.5, (HD,))
    return jnp.where(signs, 1.0, -1.0).astype(jnp.float32)


def aligned_strengths(key):
    picked = jax.random.randint(jax.random.fold_in(key, 7102), (RESIDENT,), 0, 8)
    target = 120.0 + 70.0 * picked.astype(jnp.float32)
    strength = target / (cache_strength * HD * query_scale)
    return jnp.where(picked < 4, strength, 0.0)


def draw_queries(key, part):
    plain = jnp.clip(jax.random.normal(jax.random.fold_in(key, 7201), (RESIDENT, QH * HD), jnp.float32), -6.0, 6.0)
    pattern = jnp.tile(common_pattern(key), QH)
    strength = aligned_strengths(key)
    plain = jnp.where(strength[:, None] > 0.0, strength[:, None] * pattern[None, :], plain)
    return plain.astype(jnp.bfloat16)


def draw_new_kv(key, part):
    plain = jnp.clip(jax.random.normal(jax.random.fold_in(key, 7301), (RESIDENT, KVH, 2, HD), jnp.float32), -6.0, 6.0)
    pattern = common_pattern(key)
    strength = aligned_strengths(key)
    safe = jnp.maximum(strength, 1.0)
    level = cache_strength - 2.0 / (safe * HD * query_scale)
    aligned = jnp.broadcast_to((level[:, None] * pattern[None, :])[:, None, :], (RESIDENT, KVH, HD))
    keys = jnp.where(strength[:, None, None] > 0.0, aligned, plain[:, :, 0, :])
    plain = jnp.stack([keys, plain[:, :, 1, :]], axis=2)
    return plain.astype(jnp.bfloat16)


def draw_k_cache(key, part):
    plain = jnp.clip(jax.random.normal(jax.random.fold_in(key, 7401), (PAIRS, CACHE_LEN, HD), jnp.float32), -6.0, 6.0)
    pattern = common_pattern(key)
    first = jnp.broadcast_to(cache_strength * pattern[None, None, :], (PAIRS, 1, HD))
    plain = jnp.concatenate([first, plain[:, 1:, :]], axis=1)
    return plain.astype(jnp.bfloat16)


def touch_ends(entries, key, low, largest):
    index_at = [jax.random.randint(jax.random.fold_in(key, axis), (), 0, length) for axis, length in enumerate(entries.shape)]
    widest = entries.shape.index(max(entries.shape))
    beside = index_at[:widest] + [(index_at[widest] + 1) % entries.shape[widest]] + index_at[widest + 1:]
    return entries.at[tuple(index_at)].set(low).at[tuple(beside)].set(largest)


def levels(stream_key, shape, shards, least, largest):
    factor_of = 1.0
    for dim, parts in shards:
        draws = jax.random.uniform(jax.random.fold_in(jax.random.fold_in(stream_key, 6), dim), (parts,), jnp.float32, least / len(shards), largest / len(shards))
        factor_of = factor_of * jnp.repeat(jnp.exp(draws), shape[dim] // parts).reshape((-1,) + (1,) * (len(shape) - 1 - dim))
    return factor_of


def gaussian(key, extent, spread, most, shards=(), kind=jnp.bfloat16):
    gain = levels(key, extent, shards, -0.22, 0.18) if shards else 1.0
    entries = jax.random.normal(key, extent, jnp.float32) * spread * gain
    return jnp.minimum(jnp.maximum(entries, -most), most).astype(kind)


def setup_inputs(seed: int = 0, part: int = 0) -> dict:
    key_list = jax.random.split(jax.random.key(seed), 9)
    part_keys = jax.random.split(jax.random.fold_in(key_list[8], part), 9)
    prompt_kv = gaussian(part_keys[0], (PROMPT, KV_ROWS, HD), 1.0, 6.0, ((0, 256),))
    prompt_length = jax.random.randint(part_keys[1], (1,), PROMPT // 2, PROMPT + 1).astype(jnp.int32)
    queries = draw_queries(jax.random.fold_in(jax.random.fold_in(key_list[8], part), 71), part)
    new_kv = draw_new_kv(jax.random.fold_in(jax.random.fold_in(key_list[8], part), 71), part)
    k_cache = draw_k_cache(jax.random.fold_in(jax.random.fold_in(key_list[8], part), 71), part)
    v_cache = gaussian(part_keys[5], (PAIRS, CACHE_LEN, HD), 1.0, 6.0, ((0, 32), (1, 8)))
    lengths = touch_ends(jax.random.randint(part_keys[6], (RESIDENT,), CACHE_LEN // 2 + 1, CACHE_LEN + 1), jax.random.fold_in(part_keys[6], 1), CACHE_LEN // 2 + 1, CACHE_LEN).astype(jnp.int32)
    slots = jax.random.permutation(part_keys[7], RESIDENT).astype(jnp.int32)
    return {"prompt_kv": prompt_kv, "prompt_length": prompt_length, "queries": queries, "new_kv": new_kv, "k_cache": k_cache, "v_cache": v_cache, "lengths": lengths, "slots": slots}


query_scale = 168.0 ** -0.5
negative = -1.0e30


def reference(prompt_kv, prompt_length, queries, new_kv, k_cache, v_cache, lengths, slots):
    position = jnp.arange(PROMPT, dtype=jnp.int32)
    kept = jnp.where((position < prompt_length[0])[:, None, None], prompt_kv, jnp.zeros_like(prompt_kv))
    blocks = kept.reshape(N_SEQ, N_TP, BLOCK, KV_ROWS, HD)
    prompt_owned = jnp.transpose(blocks, (1, 0, 2, 3, 4)).reshape(PROMPT, KV_ROWS, HD)

    rows = jnp.arange(PAIRS, dtype=jnp.int32)
    head_of = rows // RESIDENT
    slot_of = rows % RESIDENT
    match = slots[None, :] == slot_of[:, None]
    sequence = jnp.sum(jnp.where(match, jnp.arange(RESIDENT, dtype=jnp.int32)[None, :], 0), axis=1).astype(jnp.int32)
    grouped = queries.reshape(RESIDENT, KVH, GROUP, HD)
    query_rows = grouped[sequence, head_of].astype(jnp.float32)
    own = new_kv[sequence, head_of]
    own_key = own[:, 0].astype(jnp.float32)
    own_value = own[:, 1].astype(jnp.float32)
    live_len = lengths[sequence]

    scores = jnp.einsum("rgd,rpd->rgp", query_rows, k_cache.astype(jnp.float32)) * query_scale
    own_score = jnp.einsum("rgd,rd->rg", query_rows, own_key) * query_scale
    cache_pos = jnp.arange(CACHE_LEN, dtype=jnp.int32)
    live = cache_pos[None, None, :] < live_len[:, None, None]
    masked = jnp.where(live, scores, negative)
    top = jnp.maximum(jnp.max(masked, axis=2), own_score)
    weights = jnp.where(live, jnp.exp(masked - top[..., None]), 0.0)
    rounded = lax.optimization_barrier(weights.astype(jnp.bfloat16))
    summed = jnp.einsum("rgp,rpd->rgd", rounded.astype(jnp.float32), v_cache.astype(jnp.float32))
    own_weight = jnp.exp(own_score - top)
    total = jnp.sum(weights, axis=2) + own_weight
    summed = summed + own_weight[..., None] * own_value[:, None, :]
    attended = (summed / total[..., None]).astype(jnp.bfloat16).reshape(PAIRS, GROUP * HD)
    return prompt_owned, attended
```

```python
import jax
import jax.numpy as jnp
from jax import lax
from jax.experimental import pallas as pl
from jax.experimental.pallas import tpu as pltpu
from jax.sharding import PartitionSpec as P

query_scale = 168.0 ** (-0.5)
negative = -1e30


def regroup_kernel(n, x_ref, o_ref, own, send_sem, recv_sems, up_sems, own_sem):
    block = x_ref.shape[0]
    me = lax.axis_index("seq")
    v = lax.rem(me + n - 1, n)

    def place(w):
        return lax.rem(w + 1, n)

    barrier = pltpu.get_barrier_semaphore()

    @pl.when(v > 0)
    def _():
        pl.semaphore_wait(barrier, 1)

    @pl.when(v < n - 1)
    def _():
        pl.semaphore_signal(barrier, inc=1, device_id={"seq": place(v + 1)})

    fetch = pltpu.make_async_copy(x_ref.at[:, me], own, own_sem)
    fetch.start()

    def copy_to(w):
        to = place(w)
        return pltpu.make_async_remote_copy(
            src_ref=x_ref.at[:, to],
            dst_ref=o_ref.at[me],
            send_sem=send_sem,
            recv_sem=recv_sems.at[me],
            device_id={"seq": to},
        )

    @pl.loop(0, v)
    def _(w):
        pl.semaphore_signal(up_sems.at[v], inc=1, device_id={"seq": place(w)})

    @pl.loop(0, v)
    def _(k):
        copy_to(v - 1 - k).start()

    @pl.loop(v + 1, n)
    def _(w):
        pl.semaphore_wait(up_sems.at[w], 1)
        copy_to(w).start()

    fetch.wait()
    keep = pltpu.make_async_copy(own, o_ref.at[me], own_sem)
    keep.start()

    @pl.loop(1, n)
    def _(k):
        src = lax.rem(me + k, n)
        pltpu.make_async_copy(o_ref.at[src], o_ref.at[src], recv_sems.at[src]).wait()

    pltpu.make_async_copy(o_ref.at[pl.ds(0, n - 1)], o_ref.at[pl.ds(0, n - 1)], send_sem).wait()
    keep.wait()


def regroup(x, n):
    block, _, rows, width = x.shape
    return pl.pallas_call(
        lambda *refs: regroup_kernel(n, *refs),
        out_shape=jax.ShapeDtypeStruct((n, block, rows, width), x.dtype),
        in_specs=[pl.BlockSpec(memory_space=pl.ANY)],
        out_specs=pl.BlockSpec(memory_space=pl.ANY),
        scratch_shapes=[
            pltpu.VMEM((block, rows, width), x.dtype),
            pltpu.SemaphoreType.DMA,
            pltpu.SemaphoreType.DMA((n,)),
            pltpu.SemaphoreType.REGULAR((n,)),
            pltpu.SemaphoreType.DMA,
        ],
        compiler_params=pltpu.CompilerParams(collective_id=0, has_side_effects=True),
    )(x)


def collected_together(shard, axis):
    leaves = jax.tree.leaves(shard)
    sequence = sorted(range(len(leaves)), key=lambda k: -leaves[k].size)
    width = (1, *leaves[sequence[0]].shape)[-1]
    lines = [
        jnp.pad(leaves[k].reshape(-1), (0, -leaves[k].size % width)).reshape(-1, width)
        for k in sequence
    ]
    both, at, found = (lax.all_gather(jnp.concatenate(lines), axis), 0, {})
    for k, line in zip(sequence, lines):
        section = both[:, at : at + len(line)].reshape(len(both), -1)
        found[k] = section[:, : leaves[k].size].reshape(-1, *leaves[k].shape)
        at += len(line)
    numbers = iter(range(len(leaves)))
    return jax.tree.map(lambda _: found[next(numbers)], shard)


def joined(shard, axis, combine):
    everything = collected_together(shard, axis)
    leading = jax.tree.map(lambda part: part[0], everything)

    def step(k, so_far):
        return combine(so_far, jax.tree.map(lambda part: part[k], everything))

    return lax.fori_loop(1, lax.axis_size(axis), step, leading)


def combine_parts(first, second):
    upper = jnp.maximum(first[0], second[0])
    scale_one = jnp.exp(first[0] - upper)
    scale_two = jnp.exp(second[0] - upper)
    total = first[1] * scale_one + second[1] * scale_two
    summed = first[2] * scale_one[..., None] + second[2] * scale_two[..., None]
    return (upper, total, summed)


def per_device(prompt_kv, prompt_length, queries, new_kv, k_cache, v_cache, lengths, slots):
    block = prompt_kv.shape[0]
    n = lax.axis_size("seq")
    rows_each = prompt_kv.shape[1] // n
    width = prompt_kv.shape[2]
    landed = regroup(prompt_kv.reshape(block, n, rows_each, width), n)
    start = (jnp.arange(n, dtype=jnp.int32) * lax.axis_size("tp") + lax.axis_index("tp")) * block
    position = start[:, None] + jnp.arange(block, dtype=jnp.int32)
    live_prompt = (position < prompt_length[0])[:, :, None, None]
    prompt_owned = jnp.where(live_prompt, landed, jnp.zeros_like(landed))
    prompt_owned = prompt_owned.reshape(n * block, rows_each, width)
    resident = lengths.shape[0]
    pair_rows = k_cache.shape[0]
    span = k_cache.shape[1]
    width = k_cache.shape[2]
    heads = new_kv.shape[1]
    group = queries.shape[1] // (heads * width)
    rows = lax.axis_index("seq") * pair_rows + jnp.arange(pair_rows, dtype=jnp.int32)
    head_of = rows // resident
    slot_of = rows % resident
    match = slots[None, :] == slot_of[:, None]
    sequence = jnp.sum(jnp.where(match, jnp.arange(resident, dtype=jnp.int32)[None, :], 0), axis=1)
    grouped = queries.reshape(resident, heads, group, width)
    query_rows = grouped[sequence, head_of]
    own = new_kv[sequence, head_of]
    own_key = own[:, 0]
    own_value = own[:, 1].astype(jnp.float32)
    live_len = lengths[sequence]
    scores = (
        jnp.einsum("rgd,rpd->rgp", query_rows, k_cache, preferred_element_type=jnp.float32)
        * query_scale
    )
    own_score = (
        jnp.einsum("rgd,rd->rg", query_rows, own_key, preferred_element_type=jnp.float32)
        * query_scale
    )
    cache_pos = lax.axis_index("tp") * span + jnp.arange(span, dtype=jnp.int32)
    live = cache_pos[None, None, :] < live_len[:, None, None]
    masked = jnp.where(live, scores, negative)
    local_top = jnp.max(masked, axis=2)
    weights = jnp.where(live, jnp.exp(masked - local_top[..., None]), 0.0)
    partial_value = jnp.einsum(
        "rgp,rpd->rgd", weights.astype(jnp.bfloat16), v_cache, preferred_element_type=jnp.float32
    )
    upper, total, summed = joined(
        (local_top, jnp.sum(weights, axis=2), partial_value), "tp", combine_parts
    )
    overall = jnp.maximum(upper, own_score)
    rescale = jnp.exp(upper - overall)
    own_weight = jnp.exp(own_score - overall)
    total = total * rescale + own_weight
    summed = summed * rescale[..., None] + own_weight[..., None] * own_value[:, None, :]
    attended = (summed / total[..., None]).astype(jnp.bfloat16).reshape(pair_rows, group * width)
    return (prompt_owned, attended)


def solution(mesh):
    in_specs = (
        P(("groups", "seq", "tp"), None, None),
        P("groups"),
        P("groups", None),
        P("groups", None, None, None),
        P(("groups", "seq"), "tp", None),
        P(("groups", "seq"), "tp", None),
        P("groups"),
        P("groups"),
    )
    out_specs = (P(("groups", "tp"), "seq", None), P(("groups", "seq"), None))
    return jax.shard_map(
        per_device, mesh=mesh, in_specs=in_specs, out_specs=out_specs, check_vma=False
    )
```

```python
import jax
import jax.numpy as jnp
from jax import lax
from jax.experimental import pallas as pl
from jax.experimental.pallas import tpu as pltpu
from jax.sharding import PartitionSpec as P

query_scale = 168.0 ** (-0.5)
negative = -1e30
residue = 4


def signal(semaphore, axis, to):
    pl.semaphore_signal(semaphore, inc=1, device_id={axis: to})


def step_kernel(
    n,
    m,
    x_ref,
    length_ref,
    q_ref,
    new_ref,
    k_ref,
    v_ref,
    lengths_ref,
    slots_ref,
    out_ref,
    att_ref,
    land,
    kept,
    k_vm,
    v_vm,
    q_vm,
    new_vm,
    parts,
    send_sem,
    cross_sem,
    part_send_sem,
    own_sem,
    keep_sem,
    in_sems,
    recv_sems,
    part_sems,
    up_sems,
    token_sem,
    ring_sem,
    all_sem,
):
    me = lax.axis_index("seq")
    my = lax.axis_index("tp")
    half = n // 2
    place = lax.rem(me, half)
    gated = half - 1 - place
    block, _, rows, width = x_ref.shape

    barrier = pltpu.get_barrier_semaphore()

    @pl.when(me > 0)
    def _():
        pl.semaphore_wait(barrier, 1)

    @pl.when(me < n - 1)
    def _():
        signal(barrier, "seq", me + 1)

    @pl.when(me == 0)
    def _():
        @pl.loop(1, m)
        def _(t):
            signal(barrier, "tp", lax.rem(my + t, m))

    @pl.loop(0, me)
    def _(w):
        signal(up_sems.at[me], "seq", me - 1 - w)

    def copy_to(to, semaphore):
        return pltpu.make_async_remote_copy(
            src_ref=x_ref.at[:, to],
            dst_ref=land.at[me],
            send_sem=semaphore,
            recv_sem=recv_sems.at[me],
            device_id={"seq": to},
        )

    def send_down(low, high, semaphore):
        @pl.loop(low, high)
        def _(w):
            copy_to(w, semaphore).start()

    def send_up(low, high, semaphore):
        @pl.loop(low, high)
        def _(w):
            pl.semaphore_wait(up_sems.at[w], 1)
            copy_to(w, semaphore).start()

    def sent(count, semaphore):
        @pl.loop(0, count)
        def _(w):
            pltpu.make_async_copy(land.at[0], land.at[0], semaphore).wait()

    pairs, span = k_vm.shape[:2]
    resident = q_vm.shape[0]
    group = q_vm.shape[1] // width
    lines = pairs * group
    head = (me * pairs) // resident
    per_tile = new_vm.shape[1]
    new_row = lax.rem(head * 2, per_tile)
    new_tile = pl.multiple_of(head * 2 - new_row, per_tile)
    q_column = pl.multiple_of(head * (group * width), group * width)
    fetches = (
        pltpu.make_async_copy(x_ref.at[:, me], land.at[me], own_sem),
        pltpu.make_async_copy(k_ref, k_vm, in_sems.at[0]),
        pltpu.make_async_copy(v_ref, v_vm, in_sems.at[1]),
        pltpu.make_async_copy(q_ref.at[:, pl.ds(q_column, group * width)], q_vm, in_sems.at[2]),
        pltpu.make_async_copy(new_ref.at[:, pl.ds(new_tile, per_tile)], new_vm, in_sems.at[3]),
    )
    line = lax.broadcasted_iota(jnp.int32, (lines, 1), 0)

    def sequence_of(r):
        slot = lax.rem(me * pairs + r, resident)
        found = jnp.int32(0)
        for b in range(resident):
            found = found + jnp.where(slots_ref[b] == slot, b, 0)
        return found

    def chosen():
        which = lax.broadcasted_iota(jnp.int32, (resident, 1), 0)
        tile = lax.broadcasted_iota(jnp.int32, (per_tile, 1), 0)
        q_all = q_vm[...].astype(jnp.float32)
        query = jnp.zeros((lines, width), jnp.float32)
        own_key = jnp.zeros((lines, width), jnp.float32)
        own_value = jnp.zeros((lines, width), jnp.float32)
        live_len = jnp.zeros((lines, 1), jnp.int32)
        for r in range(pairs):
            b = sequence_of(r)
            one = jnp.sum(jnp.where(which == b, q_all, 0.0), axis=0, keepdims=True)
            for k in range(group):
                query = jnp.where(line == k * pairs + r, one[:, k * width : (k + 1) * width], query)
            mine = lax.rem(line, pairs) == r
            new = jnp.zeros((per_tile, width), jnp.float32)
            length = jnp.int32(0)
            for s in range(resident):
                new = jnp.where(b == s, new_vm[s].astype(jnp.float32), new)
                length = jnp.where(b == s, lengths_ref[s], length)
            key = jnp.sum(jnp.where(tile == new_row, new, 0.0), axis=0, keepdims=True)
            value = jnp.sum(jnp.where(tile == new_row + 1, new, 0.0), axis=0, keepdims=True)
            own_key = jnp.where(mine, key, own_key)
            own_value = jnp.where(mine, value, own_value)
            live_len = jnp.where(mine, length, live_len)
        own = jnp.sum(query * own_key, axis=1, keepdims=True) * query_scale
        return query, own, own_value, live_len

    def attend():
        for fetch in fetches[1:]:
            fetch.wait()
        query, _, _, live_len = chosen()
        query = query.astype(jnp.bfloat16)
        scores = jnp.zeros((lines, span), jnp.float32)
        for r in range(pairs):
            part = lax.dot_general(
                query, k_vm[r], (((1,), (1,)), ((), ())), preferred_element_type=jnp.float32
            )
            scores = jnp.where(lax.rem(line, pairs) == r, part, scores)
        position = my * span + lax.broadcasted_iota(jnp.int32, (lines, span), 1)
        live = position < live_len
        masked = jnp.where(live, scores * query_scale, negative)
        top = jnp.max(masked, axis=1, keepdims=True)
        weights = jnp.where(live, jnp.exp(masked - top), 0.0)
        total = jnp.sum(weights, axis=1, keepdims=True)
        rounded = weights.astype(jnp.bfloat16)
        summed = jnp.zeros((lines, width), jnp.float32)
        for r in range(pairs):
            part = jnp.dot(rounded, v_vm[r], preferred_element_type=jnp.float32)
            summed = jnp.where(lax.rem(line, pairs) == r, part, summed)
        parts[my, 0] = summed
        parts[my, 1] = jnp.broadcast_to(top, (lines, width))
        parts[my, 2] = jnp.broadcast_to(total, (lines, width))

    for fetch in fetches:
        fetch.start()

    @pl.when(me < half)
    def _():
        send_down(0, me, send_sem)

    @pl.when(me >= half)
    def _():
        send_down(0, place + 1, send_sem)
        send_down(half, me, send_sem)
        send_down(place + 1, half, cross_sem)

    attend()

    @pl.when(me < half)
    def _():
        send_up(me + 1, half, send_sem)
        send_up(half, half + place + 1, send_sem)

        @pl.when(place > 0)
        def _():
            pl.semaphore_wait(token_sem, 1)

        send_up(half + place + 1, n, cross_sem)
        sent(jnp.maximum(gated - residue, 0), cross_sem)

        @pl.when(place < half - 1)
        def _():
            signal(token_sem, "seq", me + 1)

    @pl.when(me >= half)
    def _():
        send_up(me + 1, n, send_sem)

    @pl.when(me == 0)
    def _():
        pl.semaphore_wait(barrier, m - 1)

        @pl.loop(1, m)
        def _(t):
            signal(ring_sem, "tp", lax.rem(my + t, m))

        pl.semaphore_wait(ring_sem, m - 1)

        @pl.loop(1, n)
        def _(w):
            signal(all_sem, "seq", w)

    @pl.when(me > 0)
    def _():
        pl.semaphore_wait(all_sem, 1)

    def part_to(t):
        return pltpu.make_async_remote_copy(
            src_ref=parts.at[my],
            dst_ref=parts.at[my],
            send_sem=part_send_sem,
            recv_sem=part_sems.at[my],
            device_id={"tp": lax.rem(my + t, m)},
        )

    @pl.loop(1, m)
    def _(t):
        part_to(t).start()

    @pl.loop(1, m)
    def _(t):
        other = lax.rem(my + t, m)
        pltpu.make_async_copy(parts.at[other], parts.at[other], part_sems.at[other]).wait()

    _, own, own_value, _ = chosen()
    overall = jnp.broadcast_to(own, (lines, width))
    for t in range(m):
        overall = jnp.maximum(overall, parts[t, 1])
    own_weight = jnp.exp(own - overall)
    summed = own_weight * own_value
    total = own_weight
    for t in range(m):
        scale = jnp.exp(parts[t, 1] - overall)
        summed = summed + parts[t, 0] * scale
        total = total + parts[t, 2] * scale
    att_ref[...] = summed / total

    def keep(s):
        start = (s * m + my) * block
        position = start + lax.broadcasted_iota(jnp.int32, (block, rows, width), 0)
        arrived = land[s].astype(jnp.float32)
        kept[s] = jnp.where(position < length_ref[0], arrived, 0.0).astype(kept.dtype)
        pltpu.make_async_copy(kept.at[s], out_ref.at[s], keep_sem).start()

    fetches[0].wait()
    keep(me)

    @pl.loop(1, n)
    def _(w):
        s = lax.rem(me + w, n)
        pltpu.make_async_copy(land.at[s], land.at[s], recv_sems.at[s]).wait()
        keep(s)

    sent(n - 1 - gated, send_sem)

    @pl.when(me < half)
    def _():
        sent(jnp.minimum(gated, residue), cross_sem)

    @pl.when(me >= half)
    def _():
        sent(gated, cross_sem)

    @pl.loop(1, m)
    def _(t):
        pltpu.make_async_copy(parts.at[0], parts.at[0], part_send_sem).wait()

    pltpu.make_async_copy(kept, out_ref, keep_sem).wait()


def finish_kernel(owned_ref, att_ref, out_ref, attended_ref, held, in_sems, out_sem):
    pieces = in_sems.shape[0]
    each = owned_ref.shape[0] // pieces
    pairs, lanes = attended_ref.shape
    width = att_ref.shape[1]

    def fetch(i):
        at = pl.ds(i * each, each)
        return pltpu.make_async_copy(owned_ref.at[at], held.at[at], in_sems.at[i])

    for i in range(pieces):
        fetch(i).start()
    for k in range(lanes // width):
        lines = att_ref[k * pairs : (k + 1) * pairs, :]
        attended_ref[:, k * width : (k + 1) * width] = lines.astype(attended_ref.dtype)
    for i in range(pieces):
        fetch(i).wait()
        at = pl.ds(i * each, each)
        pltpu.make_async_copy(held.at[at], out_ref.at[at], out_sem).start()
    pltpu.make_async_copy(held, out_ref, out_sem).wait()


def per_device(prompt_kv, prompt_length, queries, new_kv, k_cache, v_cache, lengths, slots):
    n = lax.axis_size("seq")
    m = lax.axis_size("tp")
    block, kv_rows, width = prompt_kv.shape
    rows = kv_rows // n
    resident, heads = new_kv.shape[:2]
    pairs, span, _ = k_cache.shape
    group = queries.shape[1] // (heads * width)
    lines = pairs * group
    anywhere = pl.BlockSpec(memory_space=pl.ANY)
    scalars = pl.BlockSpec(memory_space=pltpu.SMEM)
    vector = pl.BlockSpec(memory_space=pltpu.VMEM)
    dma, regular = pltpu.SemaphoreType.DMA, pltpu.SemaphoreType.REGULAR
    owned, attended = pl.pallas_call(
        lambda *refs: step_kernel(n, m, *refs),
        out_shape=(
            jax.ShapeDtypeStruct((n, block, rows, width), prompt_kv.dtype),
            jax.ShapeDtypeStruct((lines, width), jnp.float32),
        ),
        in_specs=[anywhere, scalars, anywhere, anywhere, anywhere, anywhere, scalars, scalars],
        out_specs=(anywhere, vector),
        scratch_shapes=[
            pltpu.VMEM((n, block, rows, width), prompt_kv.dtype),
            pltpu.VMEM((n, block, rows, width), prompt_kv.dtype),
            pltpu.VMEM(k_cache.shape, k_cache.dtype),
            pltpu.VMEM(v_cache.shape, v_cache.dtype),
            pltpu.VMEM((resident, group * width), queries.dtype),
            pltpu.VMEM((resident, 8, width), new_kv.dtype),
            pltpu.VMEM((m, 3, lines, width), jnp.float32),
            dma,
            dma,
            dma,
            dma,
            dma,
            dma((4,)),
            dma((n,)),
            dma((m,)),
            regular((n,)),
            regular,
            regular,
            regular,
        ],
        compiler_params=pltpu.CompilerParams(collective_id=0, has_side_effects=True),
    )(
        prompt_kv.reshape(block, n, rows, width),
        prompt_length,
        queries,
        new_kv.reshape(resident, heads * 2, width),
        k_cache,
        v_cache,
        lengths,
        slots,
    )
    return pl.pallas_call(
        finish_kernel,
        out_shape=(
            jax.ShapeDtypeStruct((n * block, rows, width), prompt_kv.dtype),
            jax.ShapeDtypeStruct((pairs, group * width), jnp.bfloat16),
        ),
        in_specs=[anywhere, vector],
        out_specs=(anywhere, vector),
        scratch_shapes=[pltpu.VMEM((n * block, rows, width), prompt_kv.dtype), dma((8,)), dma],
    )(owned.reshape(n * block, rows, width), attended)


def solution(mesh):
    in_specs = (
        P(("groups", "seq", "tp"), None, None),
        P("groups"),
        P("groups", None),
        P("groups", None, None, None),
        P(("groups", "seq"), "tp", None),
        P(("groups", "seq"), "tp", None),
        P("groups"),
        P("groups"),
    )
    out_specs = (P(("groups", "tp"), "seq", None), P(("groups", "seq"), None))
    return jax.shard_map(
        per_device, mesh=mesh, in_specs=in_specs, out_specs=out_specs, check_vma=False
    )
```

```python
import jax
import jax.numpy as jnp
from jax import lax
from jax.experimental import pallas as pl
from jax.experimental.pallas import tpu as pltpu
from jax.sharding import PartitionSpec as P

query_scale = 168.0 ** (-0.5)
negative = -1e30
leaders = ((0, 2), (1, 2), (2, 3), (3, 3), (4, 3), (5, 4), (6, 4), (7, 4))
herald = None


def signal(semaphore, axis, to):
    pl.semaphore_signal(semaphore, inc=1, device_id={axis: to})


def step_kernel(
    n,
    m,
    x_ref,
    length_ref,
    q_ref,
    new_ref,
    k_ref,
    v_ref,
    lengths_ref,
    slots_ref,
    out_ref,
    att_ref,
    land,
    kept,
    k_vm,
    v_vm,
    q_vm,
    new_vm,
    parts,
    send_sem,
    cross_sem,
    part_send_sem,
    length_sm,
    own_sem,
    keep_sem,
    in_sems,
    recv_sems,
    part_sems,
    up_sems,
    token_sem,
    late_sem,
    ring_sem,
    all_sem,
):
    me = lax.axis_index("seq")
    my = lax.axis_index("tp")
    half = n // 2
    place = lax.rem(me, half)
    late = (lax.axis_index("groups") == 0) & (my == 0)
    first = late.astype(jnp.int32)
    gated = jnp.where(me >= first, half - 1 - place, 0)
    leading = jnp.bool_(False)
    left = jnp.int32(0)
    for leader, residue in leaders:
        here = me == leader + first
        leading = leading | here
        left = jnp.where(here, residue, left)
    block, _, rows, width = x_ref.shape

    barrier = pltpu.get_barrier_semaphore()

    @pl.when(me > first)
    def _():
        pl.semaphore_wait(barrier, 1)

    @pl.when((me < n - 1) & ((me >= first) | late))
    def _():
        signal(barrier, "seq", me + 1)

    @pl.when(me == 0)
    def _():
        @pl.loop(1, m)
        def _(t):
            signal(barrier, "tp", lax.rem(my + t, m))

    @pl.loop(first, jnp.maximum(me, first))
    def _(w):
        signal(up_sems.at[me], "seq", first + me - 1 - w)

    def copy_to(to, semaphore):
        return pltpu.make_async_remote_copy(
            src_ref=x_ref.at[:, to],
            dst_ref=land.at[me],
            send_sem=semaphore,
            recv_sem=recv_sems.at[me],
            device_id={"seq": to},
        )

    def send_down(low, high, semaphore):
        @pl.loop(low, high)
        def _(w):
            copy_to(w, semaphore).start()

    def send_up(low, high, semaphore):
        @pl.loop(low, high)
        def _(w):
            pl.semaphore_wait(up_sems.at[w], 1)
            copy_to(w, semaphore).start()

    def received(s):
        pltpu.make_async_copy(land.at[s], land.at[s], recv_sems.at[s]).wait()

    def sent(count, semaphore):
        @pl.loop(0, count)
        def _(w):
            pltpu.make_async_copy(land.at[0], land.at[0], semaphore).wait()

    pairs, span = k_vm.shape[:2]
    resident = q_vm.shape[0]
    group = q_vm.shape[1] // width
    lines = pairs * group
    head = (me * pairs) // resident
    per_tile = new_vm.shape[1]
    new_row = lax.rem(head * 2, per_tile)
    new_tile = pl.multiple_of(head * 2 - new_row, per_tile)
    q_column = pl.multiple_of(head * (group * width), group * width)
    fetches = (
        pltpu.make_async_copy(x_ref.at[:, me], land.at[me], own_sem),
        pltpu.make_async_copy(k_ref, k_vm, in_sems.at[0]),
        pltpu.make_async_copy(v_ref, v_vm, in_sems.at[1]),
        pltpu.make_async_copy(q_ref.at[:, pl.ds(q_column, group * width)], q_vm, in_sems.at[2]),
        pltpu.make_async_copy(new_ref.at[:, pl.ds(new_tile, per_tile)], new_vm, in_sems.at[3]),
        pltpu.make_async_copy(length_ref, length_sm, in_sems.at[4]),
    )
    line = lax.broadcasted_iota(jnp.int32, (lines, 1), 0)

    def sequence_of(r):
        slot = lax.rem(me * pairs + r, resident)
        found = jnp.int32(0)
        for b in range(resident):
            found = found + jnp.where(slots_ref[b] == slot, b, 0)
        return found

    def chosen():
        which = lax.broadcasted_iota(jnp.int32, (resident, 1), 0)
        tile = lax.broadcasted_iota(jnp.int32, (per_tile, 1), 0)
        q_all = q_vm[...].astype(jnp.float32)
        query = jnp.zeros((lines, width), jnp.float32)
        own_key = jnp.zeros((lines, width), jnp.float32)
        own_value = jnp.zeros((lines, width), jnp.float32)
        live_len = jnp.zeros((lines, 1), jnp.int32)
        for r in range(pairs):
            b = sequence_of(r)
            one = jnp.sum(jnp.where(which == b, q_all, 0.0), axis=0, keepdims=True)
            for k in range(group):
                query = jnp.where(line == k * pairs + r, one[:, k * width : (k + 1) * width], query)
            mine = lax.rem(line, pairs) == r
            new = jnp.zeros((per_tile, width), jnp.float32)
            length = jnp.int32(0)
            for s in range(resident):
                new = jnp.where(b == s, new_vm[s].astype(jnp.float32), new)
                length = jnp.where(b == s, lengths_ref[s], length)
            key = jnp.sum(jnp.where(tile == new_row, new, 0.0), axis=0, keepdims=True)
            value = jnp.sum(jnp.where(tile == new_row + 1, new, 0.0), axis=0, keepdims=True)
            own_key = jnp.where(mine, key, own_key)
            own_value = jnp.where(mine, value, own_value)
            live_len = jnp.where(mine, length, live_len)
        own = jnp.sum(query * own_key, axis=1, keepdims=True) * query_scale
        return query, own, own_value, live_len

    def attend():
        for fetch in fetches[1:]:
            fetch.wait()
        query, _, _, live_len = chosen()
        query = query.astype(jnp.bfloat16)
        scores = jnp.zeros((lines, span), jnp.float32)
        for r in range(pairs):
            part = lax.dot_general(
                query, k_vm[r], (((1,), (1,)), ((), ())), preferred_element_type=jnp.float32
            )
            scores = jnp.where(lax.rem(line, pairs) == r, part, scores)
        position = my * span + lax.broadcasted_iota(jnp.int32, (lines, span), 1)
        live = position < live_len
        masked = jnp.where(live, scores * query_scale, negative)
        top = jnp.max(masked, axis=1, keepdims=True)
        weights = jnp.where(live, jnp.exp(masked - top), 0.0)
        total = jnp.sum(weights, axis=1, keepdims=True)
        rounded = weights.astype(jnp.bfloat16)
        summed = jnp.zeros((lines, width), jnp.float32)
        for r in range(pairs):
            part = jnp.dot(rounded, v_vm[r], preferred_element_type=jnp.float32)
            summed = jnp.where(lax.rem(line, pairs) == r, part, summed)
        parts[my, 0] = summed
        parts[my, 1] = jnp.broadcast_to(top, (lines, width))
        parts[my, 2] = jnp.broadcast_to(total, (lines, width))

    for fetch in fetches:
        fetch.start()

    @pl.when(me < half)
    def _():
        send_down(first, jnp.maximum(me, first), send_sem)

    @pl.when(me >= half)
    def _():
        send_down(first, place + 1, send_sem)
        send_down(place + 1, half, cross_sem)

    attend()

    @pl.when((me < half) & (me >= first))
    def _():
        send_up(me + 1, half, send_sem)
        send_up(half, half + place + 1, send_sem)

    def greet():
        signal(up_sems.at[me], "seq", 0)
        copy_to(0, send_sem).start()

    @pl.when(late & (me > 1))
    def _():
        pl.semaphore_wait(late_sem, 1)
        greet()

    @pl.when(me < first)
    def _():
        send_up(1, n, send_sem)

    @pl.when((me < half) & (me >= first))
    def _():
        @pl.when(me > first)
        def _():
            pl.semaphore_wait(token_sem, 1)

        @pl.when(jnp.logical_not(leading) & (place < half - 1))
        def _():
            signal(token_sem, "seq", me + 1)

        send_up(half + place + 1, n, cross_sem)

        @pl.when(late & (me == 1))
        def _():
            pl.semaphore_wait(barrier, 1)

            @pl.loop(2, n)
            def _(w):
                signal(late_sem, "seq", w)

            greet()

        @pl.when(leading)
        def _():
            sent(gated - left, cross_sem)
            signal(token_sem, "seq", me + 1)

    @pl.when(me >= half)
    def _():
        if herald is not None:
            received(herald)
        send_down(half, me, send_sem)
        send_up(me + 1, n, send_sem)

    @pl.when(me == 0)
    def _():
        pl.semaphore_wait(barrier, m - 1)

        @pl.loop(1, m)
        def _(t):
            signal(ring_sem, "tp", lax.rem(my + t, m))

        pl.semaphore_wait(ring_sem, m - 1)

        @pl.loop(1, n)
        def _(w):
            signal(all_sem, "seq", w)

    @pl.when(me > 0)
    def _():
        pl.semaphore_wait(all_sem, 1)

    def part_to(t):
        return pltpu.make_async_remote_copy(
            src_ref=parts.at[my],
            dst_ref=parts.at[my],
            send_sem=part_send_sem,
            recv_sem=part_sems.at[my],
            device_id={"tp": lax.rem(my + t, m)},
        )

    @pl.loop(1, m)
    def _(t):
        part_to(t).start()

    @pl.loop(1, m)
    def _(t):
        other = lax.rem(my + t, m)
        pltpu.make_async_copy(parts.at[other], parts.at[other], part_sems.at[other]).wait()

    _, own, own_value, _ = chosen()
    overall = jnp.broadcast_to(own, (lines, width))
    for t in range(m):
        overall = jnp.maximum(overall, parts[t, 1])
    own_weight = jnp.exp(own - overall)
    summed = own_weight * own_value
    total = own_weight
    for t in range(m):
        scale = jnp.exp(parts[t, 1] - overall)
        summed = summed + parts[t, 0] * scale
        total = total + parts[t, 2] * scale
    att_ref[...] = summed / total

    def keep(s):
        start = (s * m + my) * block
        position = start + lax.broadcasted_iota(jnp.int32, (block, rows, width), 0)
        arrived = land[s].astype(jnp.float32)
        kept[s] = jnp.where(position < length_sm[0], arrived, 0.0).astype(kept.dtype)
        pltpu.make_async_copy(kept.at[s], out_ref.at[s], keep_sem).start()

    fetches[0].wait()
    keep(me)

    @pl.loop(1, n)
    def _(w):
        s = lax.rem(me + w, n)
        heard = False if herald is None else (me >= half) & (s == herald)

        @pl.when(jnp.logical_not(heard))
        def _():
            received(s)

        keep(s)

    sent(n - 1 - gated, send_sem)

    sent(jnp.where(leading, left, gated), cross_sem)

    @pl.loop(1, m)
    def _(t):
        pltpu.make_async_copy(parts.at[0], parts.at[0], part_send_sem).wait()

    pltpu.make_async_copy(kept, out_ref, keep_sem).wait()


def finish_kernel(owned_ref, att_ref, out_ref, attended_ref, held, in_sems, out_sem):
    pieces = in_sems.shape[0]
    each = owned_ref.shape[0] // pieces
    pairs, lanes = attended_ref.shape
    width = att_ref.shape[1]

    def fetch(i):
        at = pl.ds(i * each, each)
        return pltpu.make_async_copy(owned_ref.at[at], held.at[at], in_sems.at[i])

    for i in range(pieces):
        fetch(i).start()
    for k in range(lanes // width):
        lines = att_ref[k * pairs : (k + 1) * pairs, :]
        attended_ref[:, k * width : (k + 1) * width] = lines.astype(attended_ref.dtype)
    for i in range(pieces):
        fetch(i).wait()
        at = pl.ds(i * each, each)
        pltpu.make_async_copy(held.at[at], out_ref.at[at], out_sem).start()
    pltpu.make_async_copy(held, out_ref, out_sem).wait()


def per_device(prompt_kv, prompt_length, queries, new_kv, k_cache, v_cache, lengths, slots):
    n = lax.axis_size("seq")
    m = lax.axis_size("tp")
    block, kv_rows, width = prompt_kv.shape
    rows = kv_rows // n
    resident, heads = new_kv.shape[:2]
    pairs, span, _ = k_cache.shape
    group = queries.shape[1] // (heads * width)
    lines = pairs * group
    anywhere = pl.BlockSpec(memory_space=pl.ANY)
    scalars = pl.BlockSpec(memory_space=pltpu.SMEM)
    vector = pl.BlockSpec(memory_space=pltpu.VMEM)
    dma, regular = pltpu.SemaphoreType.DMA, pltpu.SemaphoreType.REGULAR
    owned, attended = pl.pallas_call(
        lambda *refs: step_kernel(n, m, *refs),
        out_shape=(
            jax.ShapeDtypeStruct((n, block, rows, width), prompt_kv.dtype),
            jax.ShapeDtypeStruct((lines, width), jnp.float32),
        ),
        in_specs=[anywhere, anywhere, anywhere, anywhere, anywhere, anywhere, scalars, scalars],
        out_specs=(anywhere, vector),
        scratch_shapes=[
            pltpu.VMEM((n, block, rows, width), prompt_kv.dtype),
            pltpu.VMEM((n, block, rows, width), prompt_kv.dtype),
            pltpu.VMEM(k_cache.shape, k_cache.dtype),
            pltpu.VMEM(v_cache.shape, v_cache.dtype),
            pltpu.VMEM((resident, group * width), queries.dtype),
            pltpu.VMEM((resident, 8, width), new_kv.dtype),
            pltpu.VMEM((m, 3, lines, width), jnp.float32),
            dma,
            dma,
            dma,
            pltpu.SMEM((1,), jnp.int32),
            dma,
            dma,
            dma((5,)),
            dma((n,)),
            dma((m,)),
            regular((n,)),
            regular,
            regular,
            regular,
            regular,
        ],
        compiler_params=pltpu.CompilerParams(collective_id=0, has_side_effects=True),
    )(
        prompt_kv.reshape(block, n, rows, width),
        prompt_length,
        queries,
        new_kv.reshape(resident, heads * 2, width),
        k_cache,
        v_cache,
        lengths,
        slots,
    )
    return pl.pallas_call(
        finish_kernel,
        out_shape=(
            jax.ShapeDtypeStruct((n * block, rows, width), prompt_kv.dtype),
            jax.ShapeDtypeStruct((pairs, group * width), jnp.bfloat16),
        ),
        in_specs=[anywhere, vector],
        out_specs=(anywhere, vector),
        scratch_shapes=[pltpu.VMEM((n * block, rows, width), prompt_kv.dtype), dma((8,)), dma],
    )(owned.reshape(n * block, rows, width), attended)


def solution(mesh):
    in_specs = (
        P(("groups", "seq", "tp"), None, None),
        P("groups"),
        P("groups", None),
        P("groups", None, None, None),
        P(("groups", "seq"), "tp", None),
        P(("groups", "seq"), "tp", None),
        P("groups"),
        P("groups"),
    )
    out_specs = (P(("groups", "tp"), "seq", None), P(("groups", "seq"), None))
    return jax.shard_map(
        per_device, mesh=mesh, in_specs=in_specs, out_specs=out_specs, check_vma=False
    )
```

```python
import jax
import jax.numpy as jnp
from jax import lax
from jax.experimental import pallas as pl
from jax.experimental.pallas import tpu as pltpu
from jax.sharding import PartitionSpec as P

query_scale = 168.0 ** (-0.5)
negative = -1e30
leaders = ((0, 2), (1, 2), (2, 2), (3, 3), (4, 3), (5, 4), (6, 4), (7, 4))
herald = None


def signal(semaphore, axis, to):
    pl.semaphore_signal(semaphore, inc=1, device_id={axis: to})


def step_kernel(
    n,
    m,
    x_ref,
    length_ref,
    q_ref,
    new_ref,
    k_ref,
    v_ref,
    lengths_ref,
    slots_ref,
    out_ref,
    att_ref,
    land,
    kept,
    k_vm,
    v_vm,
    q_vm,
    new_vm,
    parts,
    send_sem,
    cross_sem,
    part_send_sem,
    length_sm,
    own_sem,
    keep_sem,
    in_sems,
    recv_sems,
    part_sems,
    up_sems,
    token_sem,
    late_sem,
    ring_sem,
    all_sem,
):
    me = lax.axis_index("seq")
    my = lax.axis_index("tp")
    half = n // 2
    place = lax.rem(me, half)
    late = (lax.axis_index("groups") == 0) & (my == 0)
    first = late.astype(jnp.int32)
    gated = jnp.where(me >= first, half - 1 - place, 0)
    leading = jnp.bool_(False)
    left = jnp.int32(0)
    for leader, residue in leaders:
        here = me == leader + first
        leading = leading | here
        left = jnp.where(here, residue, left)
    block, _, rows, width = x_ref.shape

    barrier = pltpu.get_barrier_semaphore()

    @pl.when(me > first)
    def _():
        pl.semaphore_wait(barrier, 1)

    @pl.when((me < n - 1) & ((me >= first) | late))
    def _():
        signal(barrier, "seq", me + 1)

    @pl.when(me == 0)
    def _():
        @pl.loop(1, m)
        def _(t):
            signal(barrier, "tp", lax.rem(my + t, m))

    @pl.loop(first, jnp.maximum(me, first))
    def _(w):
        signal(up_sems.at[me], "seq", first + me - 1 - w)

    def copy_to(to, semaphore):
        return pltpu.make_async_remote_copy(
            src_ref=x_ref.at[:, to],
            dst_ref=land.at[me],
            send_sem=semaphore,
            recv_sem=recv_sems.at[me],
            device_id={"seq": to},
        )

    def send_down(low, high, semaphore):
        @pl.loop(low, high)
        def _(w):
            copy_to(w, semaphore).start()

    def send_up(low, high, semaphore):
        @pl.loop(low, high)
        def _(w):
            pl.semaphore_wait(up_sems.at[w], 1)
            copy_to(w, semaphore).start()

    def received(s):
        pltpu.make_async_copy(land.at[s], land.at[s], recv_sems.at[s]).wait()

    def sent(count, semaphore):
        @pl.loop(0, count)
        def _(w):
            pltpu.make_async_copy(land.at[0], land.at[0], semaphore).wait()

    pairs, span = k_vm.shape[:2]
    resident = q_vm.shape[0]
    group = q_vm.shape[1] // width
    lines = pairs * group
    head = (me * pairs) // resident
    per_tile = new_vm.shape[1]
    new_row = lax.rem(head * 2, per_tile)
    new_tile = pl.multiple_of(head * 2 - new_row, per_tile)
    q_column = pl.multiple_of(head * (group * width), group * width)
    fetches = (
        pltpu.make_async_copy(x_ref.at[:, me], land.at[me], own_sem),
        pltpu.make_async_copy(k_ref, k_vm, in_sems.at[0]),
        pltpu.make_async_copy(v_ref, v_vm, in_sems.at[1]),
        pltpu.make_async_copy(q_ref.at[:, pl.ds(q_column, group * width)], q_vm, in_sems.at[2]),
        pltpu.make_async_copy(new_ref.at[:, pl.ds(new_tile, per_tile)], new_vm, in_sems.at[3]),
        pltpu.make_async_copy(length_ref, length_sm, in_sems.at[4]),
    )
    line = lax.broadcasted_iota(jnp.int32, (lines, 1), 0)

    def sequence_of(r):
        slot = lax.rem(me * pairs + r, resident)
        found = jnp.int32(0)
        for b in range(resident):
            found = found + jnp.where(slots_ref[b] == slot, b, 0)
        return found

    def chosen():
        which = lax.broadcasted_iota(jnp.int32, (resident, 1), 0)
        tile = lax.broadcasted_iota(jnp.int32, (per_tile, 1), 0)
        q_all = q_vm[...].astype(jnp.float32)
        query = jnp.zeros((lines, width), jnp.float32)
        own_key = jnp.zeros((lines, width), jnp.float32)
        own_value = jnp.zeros((lines, width), jnp.float32)
        live_len = jnp.zeros((lines, 1), jnp.int32)
        for r in range(pairs):
            b = sequence_of(r)
            one = jnp.sum(jnp.where(which == b, q_all, 0.0), axis=0, keepdims=True)
            for k in range(group):
                query = jnp.where(line == k * pairs + r, one[:, k * width : (k + 1) * width], query)
            mine = lax.rem(line, pairs) == r
            new = jnp.zeros((per_tile, width), jnp.float32)
            length = jnp.int32(0)
            for s in range(resident):
                new = jnp.where(b == s, new_vm[s].astype(jnp.float32), new)
                length = jnp.where(b == s, lengths_ref[s], length)
            key = jnp.sum(jnp.where(tile == new_row, new, 0.0), axis=0, keepdims=True)
            value = jnp.sum(jnp.where(tile == new_row + 1, new, 0.0), axis=0, keepdims=True)
            own_key = jnp.where(mine, key, own_key)
            own_value = jnp.where(mine, value, own_value)
            live_len = jnp.where(mine, length, live_len)
        own = jnp.sum(query * own_key, axis=1, keepdims=True) * query_scale
        return query, own, own_value, live_len

    def attend():
        for fetch in fetches[1:]:
            fetch.wait()
        query, _, _, live_len = chosen()
        query = query.astype(jnp.bfloat16)
        scores = jnp.zeros((lines, span), jnp.float32)
        for r in range(pairs):
            part = lax.dot_general(
                query, k_vm[r], (((1,), (1,)), ((), ())), preferred_element_type=jnp.float32
            )
            scores = jnp.where(lax.rem(line, pairs) == r, part, scores)
        position = my * span + lax.broadcasted_iota(jnp.int32, (lines, span), 1)
        live = position < live_len
        masked = jnp.where(live, scores * query_scale, negative)
        top = jnp.max(masked, axis=1, keepdims=True)
        weights = jnp.where(live, jnp.exp(masked - top), 0.0)
        total = jnp.sum(weights, axis=1, keepdims=True)
        rounded = weights.astype(jnp.bfloat16)
        summed = jnp.zeros((lines, width), jnp.float32)
        for r in range(pairs):
            part = jnp.dot(rounded, v_vm[r], preferred_element_type=jnp.float32)
            summed = jnp.where(lax.rem(line, pairs) == r, part, summed)
        parts[my, 0] = summed
        parts[my, 1] = jnp.broadcast_to(top, (lines, width))
        parts[my, 2] = jnp.broadcast_to(total, (lines, width))

    for fetch in fetches:
        fetch.start()

    @pl.when(me < half)
    def _():
        send_down(first, jnp.maximum(me, first), send_sem)

    @pl.when(me >= half)
    def _():
        send_down(first, place + 1, send_sem)
        send_down(place + 1, half, cross_sem)

    attend()

    @pl.when((me < half) & (me >= first))
    def _():
        send_up(me + 1, half, send_sem)
        send_up(half, half + place + 1, send_sem)

    def greet():
        signal(up_sems.at[me], "seq", 0)
        copy_to(0, send_sem).start()

    @pl.when(late & (me > 1))
    def _():
        pl.semaphore_wait(late_sem, 1)
        greet()

    @pl.when(me < first)
    def _():
        send_up(1, n, send_sem)

    @pl.when((me < half) & (me >= first))
    def _():
        @pl.when(me > first)
        def _():
            pl.semaphore_wait(token_sem, 1)

        @pl.when(jnp.logical_not(leading) & (place < half - 1))
        def _():
            signal(token_sem, "seq", me + 1)

        send_up(half + place + 1, n, cross_sem)

        @pl.when(late & (me == 1))
        def _():
            pl.semaphore_wait(barrier, 1)

            @pl.loop(2, n)
            def _(w):
                signal(late_sem, "seq", w)

            greet()

        @pl.when(leading)
        def _():
            sent(gated - left, cross_sem)
            signal(token_sem, "seq", me + 1)

    @pl.when(me >= half)
    def _():
        if herald is not None:
            received(herald)
        send_down(half, me, send_sem)
        send_up(me + 1, n, send_sem)

    @pl.when(me == 0)
    def _():
        pl.semaphore_wait(barrier, m - 1)

        @pl.loop(1, m)
        def _(t):
            signal(ring_sem, "tp", lax.rem(my + t, m))

        pl.semaphore_wait(ring_sem, m - 1)

        @pl.loop(1, n)
        def _(w):
            signal(all_sem, "seq", w)

    @pl.when(me > 0)
    def _():
        pl.semaphore_wait(all_sem, 1)

    def part_to(t):
        return pltpu.make_async_remote_copy(
            src_ref=parts.at[my],
            dst_ref=parts.at[my],
            send_sem=part_send_sem,
            recv_sem=part_sems.at[my],
            device_id={"tp": lax.rem(my + t, m)},
        )

    @pl.loop(1, m)
    def _(t):
        part_to(t).start()

    @pl.loop(1, m)
    def _(t):
        other = lax.rem(my + t, m)
        pltpu.make_async_copy(parts.at[other], parts.at[other], part_sems.at[other]).wait()

    _, own, own_value, _ = chosen()
    overall = jnp.broadcast_to(own, (lines, width))
    for t in range(m):
        overall = jnp.maximum(overall, parts[t, 1])
    own_weight = jnp.exp(own - overall)
    summed = own_weight * own_value
    total = own_weight
    for t in range(m):
        scale = jnp.exp(parts[t, 1] - overall)
        summed = summed + parts[t, 0] * scale
        total = total + parts[t, 2] * scale
    att_ref[...] = summed / total

    def keep(s):
        start = (s * m + my) * block
        position = start + lax.broadcasted_iota(jnp.int32, (block, rows, width), 0)
        arrived = land[s].astype(jnp.float32)
        kept[s] = jnp.where(position < length_sm[0], arrived, 0.0).astype(kept.dtype)
        pltpu.make_async_copy(kept.at[s], out_ref.at[s], keep_sem).start()

    fetches[0].wait()
    keep(me)

    @pl.loop(1, n)
    def _(w):
        s = lax.rem(me + w, n)
        heard = False if herald is None else (me >= half) & (s == herald)

        @pl.when(jnp.logical_not(heard))
        def _():
            received(s)

        keep(s)

    sent(n - 1 - gated, send_sem)

    sent(jnp.where(leading, left, gated), cross_sem)

    @pl.loop(1, m)
    def _(t):
        pltpu.make_async_copy(parts.at[0], parts.at[0], part_send_sem).wait()

    pltpu.make_async_copy(kept, out_ref, keep_sem).wait()


def finish_kernel(owned_ref, att_ref, out_ref, attended_ref, out_sem):
    pairs, lanes = attended_ref.shape
    width = att_ref.shape[1]
    write = pltpu.make_async_copy(owned_ref, out_ref, out_sem)
    write.start()
    for k in range(lanes // width):
        lines = att_ref[k * pairs : (k + 1) * pairs, :]
        attended_ref[:, k * width : (k + 1) * width] = lines.astype(attended_ref.dtype)
    write.wait()


def per_device(prompt_kv, prompt_length, queries, new_kv, k_cache, v_cache, lengths, slots):
    n = lax.axis_size("seq")
    m = lax.axis_size("tp")
    block, kv_rows, width = prompt_kv.shape
    rows = kv_rows // n
    resident, heads = new_kv.shape[:2]
    pairs, span, _ = k_cache.shape
    group = queries.shape[1] // (heads * width)
    lines = pairs * group
    anywhere = pl.BlockSpec(memory_space=pl.ANY)
    outside = pl.BlockSpec(memory_space=pltpu.HBM)
    scalars = pl.BlockSpec(memory_space=pltpu.SMEM)
    vector = pl.BlockSpec(memory_space=pltpu.VMEM)
    dma, regular = pltpu.SemaphoreType.DMA, pltpu.SemaphoreType.REGULAR
    owned, attended = pl.pallas_call(
        lambda *refs: step_kernel(n, m, *refs),
        out_shape=(
            pltpu.VMEM((n, block, rows, width), prompt_kv.dtype),
            pltpu.VMEM((lines, width), jnp.float32),
        ),
        in_specs=[anywhere, anywhere, anywhere, anywhere, anywhere, anywhere, scalars, scalars],
        out_specs=(anywhere, vector),
        scratch_shapes=[
            pltpu.VMEM((n, block, rows, width), prompt_kv.dtype),
            pltpu.VMEM((n, block, rows, width), prompt_kv.dtype),
            pltpu.VMEM(k_cache.shape, k_cache.dtype),
            pltpu.VMEM(v_cache.shape, v_cache.dtype),
            pltpu.VMEM((resident, group * width), queries.dtype),
            pltpu.VMEM((resident, 8, width), new_kv.dtype),
            pltpu.VMEM((m, 3, lines, width), jnp.float32),
            dma,
            dma,
            dma,
            pltpu.SMEM((1,), jnp.int32),
            dma,
            dma,
            dma((5,)),
            dma((n,)),
            dma((m,)),
            regular((n,)),
            regular,
            regular,
            regular,
            regular,
        ],
        compiler_params=pltpu.CompilerParams(
            collective_id=0, has_side_effects=True, vmem_limit_bytes=60 * 2**20
        ),
    )(
        prompt_kv.reshape(block, n, rows, width),
        prompt_length,
        queries,
        new_kv.reshape(resident, heads * 2, width),
        k_cache,
        v_cache,
        lengths,
        slots,
    )
    return pl.pallas_call(
        finish_kernel,
        out_shape=(
            jax.ShapeDtypeStruct((n * block, rows, width), prompt_kv.dtype),
            jax.ShapeDtypeStruct((pairs, group * width), jnp.bfloat16),
        ),
        in_specs=[anywhere, vector],
        out_specs=(outside, vector),
        scratch_shapes=[dma],
        compiler_params=pltpu.CompilerParams(vmem_limit_bytes=16 * 2**20),
    )(owned.reshape(n * block, rows, width), attended)


def solution(mesh):
    in_specs = (
        P(("groups", "seq", "tp"), None, None),
        P("groups"),
        P("groups", None),
        P("groups", None, None, None),
        P(("groups", "seq"), "tp", None),
        P(("groups", "seq"), "tp", None),
        P("groups"),
        P("groups"),
    )
    out_specs = (P(("groups", "tp"), "seq", None), P(("groups", "seq"), None))
    return jax.shard_map(
        per_device, mesh=mesh, in_specs=in_specs, out_specs=out_specs, check_vma=False
    )
```

```python
import jax
import jax.numpy as jnp
from jax import lax
from jax.experimental import pallas as pl
from jax.experimental.pallas import tpu as pltpu
from jax.sharding import PartitionSpec as P

query_scale = 168.0 ** (-0.5)
negative = -1e30
leaders = ((0, 2), (1, 2), (2, 2), (3, 2), (4, 4), (5, 4), (6, 5), (7, 2), (8, 3))
herald = None


def signal(semaphore, axis, to):
    pl.semaphore_signal(semaphore, inc=1, device_id={axis: to})


def step_kernel(
    n,
    m,
    x_ref,
    length_ref,
    q_ref,
    new_ref,
    k_ref,
    v_ref,
    lengths_ref,
    slots_ref,
    out_ref,
    att_ref,
    land,
    kept,
    held,
    k_vm,
    v_vm,
    q_vm,
    new_vm,
    parts,
    send_sem,
    cross_sem,
    part_send_sem,
    pass_sem,
    held_sems,
    length_sm,
    own_sem,
    keep_sem,
    in_sems,
    recv_sems,
    part_sems,
    up_sems,
    token_sem,
    late_sem,
    ring_sem,
    all_sem,
):
    me = lax.axis_index("seq")
    my = lax.axis_index("tp")
    half = n // 2
    place = lax.rem(me, half)
    late = (lax.axis_index("groups") == 0) & (my == 0)
    first = late.astype(jnp.int32)
    gated = jnp.where(me >= first, half - 1 - place, 0)
    leading = jnp.bool_(False)
    left = jnp.int32(0)
    for leader, residue in leaders:
        here = me == leader + first
        leading = leading | here
        left = jnp.where(here, residue, left)
    block, _, rows, width = x_ref.shape

    barrier = pltpu.get_barrier_semaphore()

    @pl.when(me > first)
    def _():
        pl.semaphore_wait(barrier, 1)

    @pl.when((me < n - 1) & ((me >= first) | late))
    def _():
        signal(barrier, "seq", me + 1)

    @pl.when(me == 0)
    def _():
        @pl.loop(1, m)
        def _(t):
            signal(barrier, "tp", lax.rem(my + t, m))

    @pl.loop(first, jnp.maximum(me, first))
    def _(w):
        signal(up_sems.at[me], "seq", first + me - 1 - w)

    def copy_to(to, semaphore):
        return pltpu.make_async_remote_copy(
            src_ref=x_ref.at[:, to],
            dst_ref=land.at[me],
            send_sem=semaphore,
            recv_sem=recv_sems.at[me],
            device_id={"seq": to},
        )

    def by(relay, to, slot):
        return pltpu.make_async_remote_copy(
            src_ref=x_ref.at[:, to],
            dst_ref=held.at[slot],
            send_sem=send_sem,
            recv_sem=held_sems.at[slot],
            device_id={"seq": relay},
        )

    def pass_on(source, to, slot):
        return pltpu.make_async_remote_copy(
            src_ref=held.at[slot],
            dst_ref=land.at[source],
            send_sem=pass_sem,
            recv_sem=recv_sems.at[source],
            device_id={"seq": to},
        )

    passes_down = (me > first) & (me <= half)
    passes_up = (me >= half - 1 + first) & (me < n - 1)

    def relay_down():
        @pl.when(passes_down)
        def _():
            pltpu.make_async_copy(held.at[0], held.at[0], held_sems.at[0]).wait()
            pass_on(me + half - 1, me - 1, 0).start()

    def relay_up():
        @pl.when(passes_up)
        def _():
            pltpu.make_async_copy(held.at[1], held.at[1], held_sems.at[1]).wait()
            pass_on(me - half + 1, me + 1, 1).start()

    def send_down(low, high, semaphore):
        @pl.loop(low, high)
        def _(w):
            copy_to(w, semaphore).start()

    def send_up(low, high, semaphore):
        @pl.loop(low, high)
        def _(w):
            pl.semaphore_wait(up_sems.at[w], 1)
            copy_to(w, semaphore).start()

    def received(s):
        pltpu.make_async_copy(land.at[s], land.at[s], recv_sems.at[s]).wait()

    def sent(count, semaphore):
        @pl.loop(0, count)
        def _(w):
            pltpu.make_async_copy(land.at[0], land.at[0], semaphore).wait()

    pairs, span = k_vm.shape[:2]
    resident = q_vm.shape[0]
    group = q_vm.shape[1] // width
    lines = pairs * group
    head = (me * pairs) // resident
    per_tile = new_vm.shape[1]
    new_row = lax.rem(head * 2, per_tile)
    new_tile = pl.multiple_of(head * 2 - new_row, per_tile)
    q_column = pl.multiple_of(head * (group * width), group * width)
    fetches = (
        pltpu.make_async_copy(x_ref.at[:, me], land.at[me], own_sem),
        pltpu.make_async_copy(k_ref, k_vm, in_sems.at[0]),
        pltpu.make_async_copy(v_ref, v_vm, in_sems.at[1]),
        pltpu.make_async_copy(q_ref.at[:, pl.ds(q_column, group * width)], q_vm, in_sems.at[2]),
        pltpu.make_async_copy(new_ref.at[:, pl.ds(new_tile, per_tile)], new_vm, in_sems.at[3]),
        pltpu.make_async_copy(length_ref, length_sm, in_sems.at[4]),
    )
    line = lax.broadcasted_iota(jnp.int32, (lines, 1), 0)

    def sequence_of(r):
        slot = lax.rem(me * pairs + r, resident)
        found = jnp.int32(0)
        for b in range(resident):
            found = found + jnp.where(slots_ref[b] == slot, b, 0)
        return found

    def chosen():
        which = lax.broadcasted_iota(jnp.int32, (resident, 1), 0)
        tile = lax.broadcasted_iota(jnp.int32, (per_tile, 1), 0)
        q_all = q_vm[...].astype(jnp.float32)
        query = jnp.zeros((lines, width), jnp.float32)
        own_key = jnp.zeros((lines, width), jnp.float32)
        own_value = jnp.zeros((lines, width), jnp.float32)
        live_len = jnp.zeros((lines, 1), jnp.int32)
        for r in range(pairs):
            b = sequence_of(r)
            one = jnp.sum(jnp.where(which == b, q_all, 0.0), axis=0, keepdims=True)
            for k in range(group):
                query = jnp.where(line == k * pairs + r, one[:, k * width : (k + 1) * width], query)
            mine = lax.rem(line, pairs) == r
            new = jnp.zeros((per_tile, width), jnp.float32)
            length = jnp.int32(0)
            for s in range(resident):
                new = jnp.where(b == s, new_vm[s].astype(jnp.float32), new)
                length = jnp.where(b == s, lengths_ref[s], length)
            key = jnp.sum(jnp.where(tile == new_row, new, 0.0), axis=0, keepdims=True)
            value = jnp.sum(jnp.where(tile == new_row + 1, new, 0.0), axis=0, keepdims=True)
            own_key = jnp.where(mine, key, own_key)
            own_value = jnp.where(mine, value, own_value)
            live_len = jnp.where(mine, length, live_len)
        own = jnp.sum(query * own_key, axis=1, keepdims=True) * query_scale
        return query, own, own_value, live_len

    def attend():
        for fetch in fetches[1:]:
            fetch.wait()
        query, _, _, live_len = chosen()
        query = query.astype(jnp.bfloat16)
        scores = jnp.zeros((lines, span), jnp.float32)
        for r in range(pairs):
            part = lax.dot_general(
                query, k_vm[r], (((1,), (1,)), ((), ())), preferred_element_type=jnp.float32
            )
            scores = jnp.where(lax.rem(line, pairs) == r, part, scores)
        position = my * span + lax.broadcasted_iota(jnp.int32, (lines, span), 1)
        live = position < live_len
        masked = jnp.where(live, scores * query_scale, negative)
        top = jnp.max(masked, axis=1, keepdims=True)
        weights = jnp.where(live, jnp.exp(masked - top), 0.0)
        total = jnp.sum(weights, axis=1, keepdims=True)
        rounded = weights.astype(jnp.bfloat16)
        summed = jnp.zeros((lines, width), jnp.float32)
        for r in range(pairs):
            part = jnp.dot(rounded, v_vm[r], preferred_element_type=jnp.float32)
            summed = jnp.where(lax.rem(line, pairs) == r, part, summed)
        parts[my, 0] = summed
        parts[my, 1] = jnp.broadcast_to(top, (lines, width))
        parts[my, 2] = jnp.broadcast_to(total, (lines, width))

    for fetch in fetches:
        fetch.start()

    @pl.when(me < half)
    def _():
        send_down(first, jnp.maximum(me, first), send_sem)

    @pl.when(me >= half)
    def _():
        @pl.when(place >= first)
        def _():
            by(place + 1, place, 0).start()

        send_down(first, jnp.maximum(place, first), send_sem)
        send_down(place + 1, half, cross_sem)

    attend()

    @pl.when((me < half) & (me >= first))
    def _():
        send_up(me + 1, half, send_sem)
        send_up(half, half + place, send_sem)
        by(half + place - 1, half + place, 1).start()
        pl.semaphore_wait(up_sems.at[half + place], 1)

    def greet():
        signal(up_sems.at[me], "seq", 0)
        copy_to(0, send_sem).start()

    @pl.when(late & (me > 1))
    def _():
        pl.semaphore_wait(late_sem, 1)
        greet()

    @pl.when(me < first)
    def _():
        send_up(1, n, send_sem)

    @pl.when((me < half) & (me >= first))
    def _():
        @pl.when(me > first)
        def _():
            pl.semaphore_wait(token_sem, 1)

        @pl.when(jnp.logical_not(leading) & (place < half - 1))
        def _():
            signal(token_sem, "seq", me + 1)

        send_up(half + place + 1, n, cross_sem)

        @pl.when(late & (me == 1))
        def _():
            pl.semaphore_wait(barrier, 1)

            @pl.loop(2, n)
            def _(w):
                signal(late_sem, "seq", w)

            greet()

        relay_down()
        relay_up()

        @pl.when(leading)
        def _():
            sent(gated - left, cross_sem)
            signal(token_sem, "seq", me + 1)

    @pl.when(me >= half)
    def _():
        if herald is not None:
            received(herald)
        send_down(half, me, send_sem)
        send_up(me + 1, n, send_sem)
        relay_down()
        relay_up()

    @pl.when(me == 0)
    def _():
        pl.semaphore_wait(barrier, m - 1)

        @pl.loop(1, m)
        def _(t):
            signal(ring_sem, "tp", lax.rem(my + t, m))

        pl.semaphore_wait(ring_sem, m - 1)

        @pl.loop(1, n)
        def _(w):
            signal(all_sem, "seq", w)

    @pl.when(me > 0)
    def _():
        pl.semaphore_wait(all_sem, 1)

    def part_to(t):
        return pltpu.make_async_remote_copy(
            src_ref=parts.at[my],
            dst_ref=parts.at[my],
            send_sem=part_send_sem,
            recv_sem=part_sems.at[my],
            device_id={"tp": lax.rem(my + t, m)},
        )

    @pl.loop(1, m)
    def _(t):
        part_to(t).start()

    @pl.loop(1, m)
    def _(t):
        other = lax.rem(my + t, m)
        pltpu.make_async_copy(parts.at[other], parts.at[other], part_sems.at[other]).wait()

    _, own, own_value, _ = chosen()
    overall = jnp.broadcast_to(own, (lines, width))
    for t in range(m):
        overall = jnp.maximum(overall, parts[t, 1])
    own_weight = jnp.exp(own - overall)
    summed = own_weight * own_value
    total = own_weight
    for t in range(m):
        scale = jnp.exp(parts[t, 1] - overall)
        summed = summed + parts[t, 0] * scale
        total = total + parts[t, 2] * scale
    att_ref[...] = summed / total

    def keep(s):
        start = (s * m + my) * block
        position = start + lax.broadcasted_iota(jnp.int32, (block, rows, width), 0)
        arrived = land[s].astype(jnp.float32)
        kept[s] = jnp.where(position < length_sm[0], arrived, 0.0).astype(kept.dtype)
        pltpu.make_async_copy(kept.at[s], out_ref.at[s], keep_sem).start()

    fetches[0].wait()
    keep(me)

    @pl.loop(1, n)
    def _(w):
        s = lax.rem(me + w, n)
        heard = False if herald is None else (me >= half) & (s == herald)

        @pl.when(jnp.logical_not(heard))
        def _():
            received(s)

        keep(s)

    sent(n - 1 - gated, send_sem)

    sent(jnp.where(leading, left, gated), cross_sem)
    sent(passes_down.astype(jnp.int32) + passes_up.astype(jnp.int32), pass_sem)

    @pl.loop(1, m)
    def _(t):
        pltpu.make_async_copy(parts.at[0], parts.at[0], part_send_sem).wait()

    pltpu.make_async_copy(kept, out_ref, keep_sem).wait()


def finish_kernel(owned_ref, att_ref, out_ref, attended_ref, out_sem):
    pairs, lanes = attended_ref.shape
    width = att_ref.shape[1]
    write = pltpu.make_async_copy(owned_ref, out_ref, out_sem)
    write.start()
    for k in range(lanes // width):
        lines = att_ref[k * pairs : (k + 1) * pairs, :]
        attended_ref[:, k * width : (k + 1) * width] = lines.astype(attended_ref.dtype)
    write.wait()


def per_device(prompt_kv, prompt_length, queries, new_kv, k_cache, v_cache, lengths, slots):
    n = lax.axis_size("seq")
    m = lax.axis_size("tp")
    block, kv_rows, width = prompt_kv.shape
    rows = kv_rows // n
    resident, heads = new_kv.shape[:2]
    pairs, span, _ = k_cache.shape
    group = queries.shape[1] // (heads * width)
    lines = pairs * group
    anywhere = pl.BlockSpec(memory_space=pl.ANY)
    outside = pl.BlockSpec(memory_space=pltpu.HBM)
    scalars = pl.BlockSpec(memory_space=pltpu.SMEM)
    vector = pl.BlockSpec(memory_space=pltpu.VMEM)
    dma, regular = pltpu.SemaphoreType.DMA, pltpu.SemaphoreType.REGULAR
    owned, attended = pl.pallas_call(
        lambda *refs: step_kernel(n, m, *refs),
        out_shape=(
            pltpu.VMEM((n, block, rows, width), prompt_kv.dtype),
            pltpu.VMEM((lines, width), jnp.float32),
        ),
        in_specs=[anywhere, anywhere, anywhere, anywhere, anywhere, anywhere, scalars, scalars],
        out_specs=(anywhere, vector),
        scratch_shapes=[
            pltpu.VMEM((n, block, rows, width), prompt_kv.dtype),
            pltpu.VMEM((n, block, rows, width), prompt_kv.dtype),
            pltpu.VMEM((2, block, rows, width), prompt_kv.dtype),
            pltpu.VMEM(k_cache.shape, k_cache.dtype),
            pltpu.VMEM(v_cache.shape, v_cache.dtype),
            pltpu.VMEM((resident, group * width), queries.dtype),
            pltpu.VMEM((resident, 8, width), new_kv.dtype),
            pltpu.VMEM((m, 3, lines, width), jnp.float32),
            dma,
            dma,
            dma,
            dma,
            dma((2,)),
            pltpu.SMEM((1,), jnp.int32),
            dma,
            dma,
            dma((5,)),
            dma((n,)),
            dma((m,)),
            regular((n,)),
            regular,
            regular,
            regular,
            regular,
        ],
        compiler_params=pltpu.CompilerParams(
            collective_id=0, has_side_effects=True, vmem_limit_bytes=60 * 2**20
        ),
    )(
        prompt_kv.reshape(block, n, rows, width),
        prompt_length,
        queries,
        new_kv.reshape(resident, heads * 2, width),
        k_cache,
        v_cache,
        lengths,
        slots,
    )
    return pl.pallas_call(
        finish_kernel,
        out_shape=(
            jax.ShapeDtypeStruct((n * block, rows, width), prompt_kv.dtype),
            jax.ShapeDtypeStruct((pairs, group * width), jnp.bfloat16),
        ),
        in_specs=[anywhere, vector],
        out_specs=(outside, vector),
        scratch_shapes=[dma],
        compiler_params=pltpu.CompilerParams(vmem_limit_bytes=16 * 2**20),
    )(owned.reshape(n * block, rows, width), attended)


def solution(mesh):
    in_specs = (
        P(("groups", "seq", "tp"), None, None),
        P("groups"),
        P("groups", None),
        P("groups", None, None, None),
        P(("groups", "seq"), "tp", None),
        P(("groups", "seq"), "tp", None),
        P("groups"),
        P("groups"),
    )
    out_specs = (P(("groups", "tp"), "seq", None), P(("groups", "seq"), None))
    return jax.shard_map(
        per_device, mesh=mesh, in_specs=in_specs, out_specs=out_specs, check_vma=False
    )
```

```python
import jax
import jax.numpy as jnp
from jax import lax
from jax.experimental import pallas as pl
from jax.experimental.pallas import tpu as pltpu
from jax.sharding import PartitionSpec as P

query_scale = 168.0 ** (-0.5)
negative = -1e30
leaders = ((0, 2), (1, 2), (2, 1), (3, 2), (4, 4), (5, 5), (6, 6), (7, 3), (8, 4))
herald = None


def signal(semaphore, axis, to):
    pl.semaphore_signal(semaphore, inc=1, device_id={axis: to})


def step_kernel(
    n,
    m,
    x_ref,
    length_ref,
    q_ref,
    new_ref,
    k_ref,
    v_ref,
    lengths_ref,
    slots_ref,
    out_ref,
    att_ref,
    land,
    kept,
    held,
    k_vm,
    v_vm,
    q_vm,
    new_vm,
    parts,
    send_sem,
    cross_sem,
    part_send_sem,
    pass_sem,
    held_sems,
    length_sm,
    own_sem,
    keep_sem,
    in_sems,
    recv_sems,
    part_sems,
    up_sems,
    token_sem,
    late_sem,
    ring_sem,
    all_sem,
):
    me = lax.axis_index("seq")
    my = lax.axis_index("tp")
    half = n // 2
    place = lax.rem(me, half)
    late = (lax.axis_index("groups") == 0) & (my == 0)
    first = late.astype(jnp.int32)
    gated = jnp.where(me >= first, half - 1 - place, 0)
    leading = jnp.bool_(False)
    left = jnp.int32(0)
    for leader, residue in leaders:
        here = me == leader + first
        leading = leading | here
        left = jnp.where(here, residue, left)
    block, _, rows, width = x_ref.shape

    barrier = pltpu.get_barrier_semaphore()

    @pl.when(me > first)
    def _():
        pl.semaphore_wait(barrier, 1)

    @pl.when((me < n - 1) & ((me >= first) | late))
    def _():
        signal(barrier, "seq", me + 1)

    @pl.when(me == 0)
    def _():
        @pl.loop(1, m)
        def _(t):
            signal(barrier, "tp", lax.rem(my + t, m))

    @pl.loop(first, jnp.maximum(me, first))
    def _(w):
        signal(up_sems.at[me], "seq", first + me - 1 - w)

    def copy_to(to, semaphore):
        return pltpu.make_async_remote_copy(
            src_ref=x_ref.at[:, to],
            dst_ref=land.at[me],
            send_sem=semaphore,
            recv_sem=recv_sems.at[me],
            device_id={"seq": to},
        )

    def by(relay, to, slot):
        return pltpu.make_async_remote_copy(
            src_ref=x_ref.at[:, to],
            dst_ref=held.at[slot],
            send_sem=send_sem,
            recv_sem=held_sems.at[slot],
            device_id={"seq": relay},
        )

    def pass_on(source, to, slot):
        return pltpu.make_async_remote_copy(
            src_ref=held.at[slot],
            dst_ref=land.at[source],
            send_sem=pass_sem,
            recv_sem=recv_sems.at[source],
            device_id={"seq": to},
        )

    passes_down = (me > first) & (me <= half)
    passes_up = (me >= half - 1 + first) & (me < n - 1)

    def relay_down():
        @pl.when(passes_down)
        def _():
            pltpu.make_async_copy(held.at[0], held.at[0], held_sems.at[0]).wait()
            pass_on(me + half - 1, me - 1, 0).start()

    def relay_up():
        @pl.when(passes_up)
        def _():
            pltpu.make_async_copy(held.at[1], held.at[1], held_sems.at[1]).wait()
            pass_on(me - half + 1, me + 1, 1).start()

    def send_down(low, high, semaphore):
        @pl.loop(low, high)
        def _(w):
            copy_to(w, semaphore).start()

    def send_up(low, high, semaphore):
        @pl.loop(low, high)
        def _(w):
            pl.semaphore_wait(up_sems.at[w], 1)
            copy_to(w, semaphore).start()

    def received(s):
        pltpu.make_async_copy(land.at[s], land.at[s], recv_sems.at[s]).wait()

    def sent(count, semaphore):
        @pl.loop(0, count)
        def _(w):
            pltpu.make_async_copy(land.at[0], land.at[0], semaphore).wait()

    pairs, span = k_vm.shape[:2]
    resident = q_vm.shape[0]
    group = q_vm.shape[1] // width
    lines = pairs * group
    head = (me * pairs) // resident
    per_tile = new_vm.shape[1]
    new_row = lax.rem(head * 2, per_tile)
    new_tile = pl.multiple_of(head * 2 - new_row, per_tile)
    q_column = pl.multiple_of(head * (group * width), group * width)
    fetches = (
        pltpu.make_async_copy(x_ref.at[:, me], land.at[me], own_sem),
        pltpu.make_async_copy(k_ref, k_vm, in_sems.at[0]),
        pltpu.make_async_copy(v_ref, v_vm, in_sems.at[1]),
        pltpu.make_async_copy(q_ref.at[:, pl.ds(q_column, group * width)], q_vm, in_sems.at[2]),
        pltpu.make_async_copy(new_ref.at[:, pl.ds(new_tile, per_tile)], new_vm, in_sems.at[3]),
        pltpu.make_async_copy(length_ref, length_sm, in_sems.at[4]),
    )
    line = lax.broadcasted_iota(jnp.int32, (lines, 1), 0)

    def sequence_of(r):
        slot = lax.rem(me * pairs + r, resident)
        found = jnp.int32(0)
        for b in range(resident):
            found = found + jnp.where(slots_ref[b] == slot, b, 0)
        return found

    def chosen():
        which = lax.broadcasted_iota(jnp.int32, (resident, 1), 0)
        tile = lax.broadcasted_iota(jnp.int32, (per_tile, 1), 0)
        q_all = q_vm[...].astype(jnp.float32)
        query = jnp.zeros((lines, width), jnp.float32)
        own_key = jnp.zeros((lines, width), jnp.float32)
        own_value = jnp.zeros((lines, width), jnp.float32)
        live_len = jnp.zeros((lines, 1), jnp.int32)
        for r in range(pairs):
            b = sequence_of(r)
            one = jnp.sum(jnp.where(which == b, q_all, 0.0), axis=0, keepdims=True)
            for k in range(group):
                query = jnp.where(line == k * pairs + r, one[:, k * width : (k + 1) * width], query)
            mine = lax.rem(line, pairs) == r
            new = jnp.zeros((per_tile, width), jnp.float32)
            length = jnp.int32(0)
            for s in range(resident):
                new = jnp.where(b == s, new_vm[s].astype(jnp.float32), new)
                length = jnp.where(b == s, lengths_ref[s], length)
            key = jnp.sum(jnp.where(tile == new_row, new, 0.0), axis=0, keepdims=True)
            value = jnp.sum(jnp.where(tile == new_row + 1, new, 0.0), axis=0, keepdims=True)
            own_key = jnp.where(mine, key, own_key)
            own_value = jnp.where(mine, value, own_value)
            live_len = jnp.where(mine, length, live_len)
        own = jnp.sum(query * own_key, axis=1, keepdims=True) * query_scale
        return query, own, own_value, live_len

    def attend():
        for fetch in fetches[1:]:
            fetch.wait()
        query, _, _, live_len = chosen()
        query = query.astype(jnp.bfloat16)
        scores = jnp.zeros((lines, span), jnp.float32)
        for r in range(pairs):
            part = lax.dot_general(
                query, k_vm[r], (((1,), (1,)), ((), ())), preferred_element_type=jnp.float32
            )
            scores = jnp.where(lax.rem(line, pairs) == r, part, scores)
        position = my * span + lax.broadcasted_iota(jnp.int32, (lines, span), 1)
        live = position < live_len
        masked = jnp.where(live, scores * query_scale, negative)
        top = jnp.max(masked, axis=1, keepdims=True)
        weights = jnp.where(live, jnp.exp(masked - top), 0.0)
        total = jnp.sum(weights, axis=1, keepdims=True)
        rounded = weights.astype(jnp.bfloat16)
        summed = jnp.zeros((lines, width), jnp.float32)
        for r in range(pairs):
            part = jnp.dot(rounded, v_vm[r], preferred_element_type=jnp.float32)
            summed = jnp.where(lax.rem(line, pairs) == r, part, summed)
        parts[my, 0] = summed
        parts[my, 1] = jnp.broadcast_to(top, (lines, width))
        parts[my, 2] = jnp.broadcast_to(total, (lines, width))

    for fetch in fetches:
        fetch.start()

    @pl.when(me < half)
    def _():
        send_down(first, jnp.maximum(me, first), send_sem)

    @pl.when(me >= half)
    def _():
        @pl.when(place >= first)
        def _():
            by(place + 1, place, 0).start()

        send_down(first, jnp.maximum(place, first), send_sem)
        send_down(place + 1, half, cross_sem)

    attend()

    @pl.when((me < half) & (me >= first))
    def _():
        send_up(me + 1, half, send_sem)
        send_up(half, half + place, send_sem)
        by(half + place - 1, half + place, 1).start()
        pl.semaphore_wait(up_sems.at[half + place], 1)

    def greet():
        signal(up_sems.at[me], "seq", 0)
        copy_to(0, send_sem).start()

    @pl.when(late & (me > 1))
    def _():
        pl.semaphore_wait(late_sem, 1)
        greet()

    @pl.when(me < first)
    def _():
        send_up(1, n, send_sem)

    @pl.when((me < half) & (me >= first))
    def _():
        @pl.when(me > first)
        def _():
            pl.semaphore_wait(token_sem, 1)

        @pl.when(jnp.logical_not(leading) & (place < half - 1))
        def _():
            signal(token_sem, "seq", me + 1)

        send_up(half + place + 1, n, cross_sem)

        @pl.when(late & (me == 1))
        def _():
            pl.semaphore_wait(barrier, 1)

            @pl.loop(2, n)
            def _(w):
                signal(late_sem, "seq", w)

            greet()

        relay_down()
        relay_up()

        @pl.when(leading)
        def _():
            sent(gated - left, cross_sem)
            signal(token_sem, "seq", me + 1)

    @pl.when(me >= half)
    def _():
        if herald is not None:
            received(herald)
        send_down(half, me, send_sem)
        send_up(me + 1, n, send_sem)
        relay_down()
        relay_up()

    @pl.when(me == 0)
    def _():
        pl.semaphore_wait(barrier, m - 1)

        @pl.loop(1, m)
        def _(t):
            signal(ring_sem, "tp", lax.rem(my + t, m))

        pl.semaphore_wait(ring_sem, m - 1)

        @pl.loop(1, n)
        def _(w):
            signal(all_sem, "seq", w)

    @pl.when(me > 0)
    def _():
        pl.semaphore_wait(all_sem, 1)

    def part_to(t):
        return pltpu.make_async_remote_copy(
            src_ref=parts.at[my],
            dst_ref=parts.at[my],
            send_sem=part_send_sem,
            recv_sem=part_sems.at[my],
            device_id={"tp": lax.rem(my + t, m)},
        )

    @pl.loop(1, m)
    def _(t):
        part_to(t).start()

    @pl.loop(1, m)
    def _(t):
        other = lax.rem(my + t, m)
        pltpu.make_async_copy(parts.at[other], parts.at[other], part_sems.at[other]).wait()

    _, own, own_value, _ = chosen()
    overall = jnp.broadcast_to(own, (lines, width))
    for t in range(m):
        overall = jnp.maximum(overall, parts[t, 1])
    own_weight = jnp.exp(own - overall)
    summed = own_weight * own_value
    total = own_weight
    for t in range(m):
        scale = jnp.exp(parts[t, 1] - overall)
        summed = summed + parts[t, 0] * scale
        total = total + parts[t, 2] * scale
    att_ref[...] = summed / total

    def keep(s):
        start = (s * m + my) * block
        position = start + lax.broadcasted_iota(jnp.int32, (block, rows, width), 0)
        arrived = land[s].astype(jnp.float32)
        kept[s] = jnp.where(position < length_sm[0], arrived, 0.0).astype(kept.dtype)
        pltpu.make_async_copy(kept.at[s], out_ref.at[s], keep_sem).start()

    fetches[0].wait()
    keep(me)

    @pl.loop(1, n)
    def _(w):
        s = lax.rem(me + w, n)
        heard = False if herald is None else (me >= half) & (s == herald)

        @pl.when(jnp.logical_not(heard))
        def _():
            received(s)

        keep(s)

    sent(n - 1 - gated, send_sem)

    sent(jnp.where(leading, left, gated), cross_sem)
    sent(passes_down.astype(jnp.int32) + passes_up.astype(jnp.int32), pass_sem)

    @pl.loop(1, m)
    def _(t):
        pltpu.make_async_copy(parts.at[0], parts.at[0], part_send_sem).wait()

    pltpu.make_async_copy(kept, out_ref, keep_sem).wait()


def finish_kernel(owned_ref, att_ref, out_ref, attended_ref, out_sem):
    pairs, lanes = attended_ref.shape
    width = att_ref.shape[1]
    write = pltpu.make_async_copy(owned_ref, out_ref, out_sem)
    write.start()
    for k in range(lanes // width):
        lines = att_ref[k * pairs : (k + 1) * pairs, :]
        attended_ref[:, k * width : (k + 1) * width] = lines.astype(attended_ref.dtype)
    write.wait()


def per_device(prompt_kv, prompt_length, queries, new_kv, k_cache, v_cache, lengths, slots):
    n = lax.axis_size("seq")
    m = lax.axis_size("tp")
    block, kv_rows, width = prompt_kv.shape
    rows = kv_rows // n
    resident, heads = new_kv.shape[:2]
    pairs, span, _ = k_cache.shape
    group = queries.shape[1] // (heads * width)
    lines = pairs * group
    anywhere = pl.BlockSpec(memory_space=pl.ANY)
    outside = pl.BlockSpec(memory_space=pltpu.HBM)
    scalars = pl.BlockSpec(memory_space=pltpu.SMEM)
    vector = pl.BlockSpec(memory_space=pltpu.VMEM)
    dma, regular = pltpu.SemaphoreType.DMA, pltpu.SemaphoreType.REGULAR
    owned, attended = pl.pallas_call(
        lambda *refs: step_kernel(n, m, *refs),
        out_shape=(
            pltpu.VMEM((n, block, rows, width), prompt_kv.dtype),
            pltpu.VMEM((lines, width), jnp.float32),
        ),
        in_specs=[anywhere, anywhere, anywhere, anywhere, anywhere, anywhere, scalars, scalars],
        out_specs=(anywhere, vector),
        scratch_shapes=[
            pltpu.VMEM((n, block, rows, width), prompt_kv.dtype),
            pltpu.VMEM((n, block, rows, width), prompt_kv.dtype),
            pltpu.VMEM((2, block, rows, width), prompt_kv.dtype),
            pltpu.VMEM(k_cache.shape, k_cache.dtype),
            pltpu.VMEM(v_cache.shape, v_cache.dtype),
            pltpu.VMEM((resident, group * width), queries.dtype),
            pltpu.VMEM((resident, 8, width), new_kv.dtype),
            pltpu.VMEM((m, 3, lines, width), jnp.float32),
            dma,
            dma,
            dma,
            dma,
            dma((2,)),
            pltpu.SMEM((1,), jnp.int32),
            dma,
            dma,
            dma((5,)),
            dma((n,)),
            dma((m,)),
            regular((n,)),
            regular,
            regular,
            regular,
            regular,
        ],
        compiler_params=pltpu.CompilerParams(
            collective_id=0, has_side_effects=True, vmem_limit_bytes=60 * 2**20
        ),
    )(
        prompt_kv.reshape(block, n, rows, width),
        prompt_length,
        queries,
        new_kv.reshape(resident, heads * 2, width),
        k_cache,
        v_cache,
        lengths,
        slots,
    )
    return pl.pallas_call(
        finish_kernel,
        out_shape=(
            jax.ShapeDtypeStruct((n * block, rows, width), prompt_kv.dtype),
            jax.ShapeDtypeStruct((pairs, group * width), jnp.bfloat16),
        ),
        in_specs=[anywhere, vector],
        out_specs=(outside, vector),
        scratch_shapes=[dma],
        compiler_params=pltpu.CompilerParams(vmem_limit_bytes=16 * 2**20),
    )(owned.reshape(n * block, rows, width), attended)


def solution(mesh):
    in_specs = (
        P(("groups", "seq", "tp"), None, None),
        P("groups"),
        P("groups", None),
        P("groups", None, None, None),
        P(("groups", "seq"), "tp", None),
        P(("groups", "seq"), "tp", None),
        P("groups"),
        P("groups"),
    )
    out_specs = (P(("groups", "tp"), "seq", None), P(("groups", "seq"), None))
    return jax.shard_map(
        per_device, mesh=mesh, in_specs=in_specs, out_specs=out_specs, check_vma=False
    )
```
